32 devices in a mesh: dp: 8 (over y, x, core), heads: 4 (over z).
Axes of the slice: x: 2, y: 2, z: 4, core: 2. Of those that a mesh axis runs over, the one named last changes fastest.
Arguments:
- inputs: bfloat16 [2048, 16, 512], P('heads', 'dp'), may hold values from -6 to 6
- lengths: int32 [16], P('dp'), may hold values from 512 to 2048, as said below
- attn_gain: bfloat16 [512], replicated, may hold values from 0.5 to 1.5
- w_query: bfloat16 [512, 512], P(None, 'heads'), may hold values from -0.25 to 0.25
- w_key: bfloat16 [512, 512], P(None, 'heads'), may hold values from -0.25 to 0.25
- w_value: bfloat16 [512, 512], P(None, 'heads'), may hold values from -0.25 to 0.25
- w_output: bfloat16 [512, 512], P('heads'), may hold values from -5 to 5
- ffn_gain: bfloat16 [512], replicated, may hold values from 0.5 to 1.5
- w_hidden: bfloat16 [512, 2048], P(None, 'heads'), may hold values from -0.25 to 0.25
- b_hidden: bfloat16 [2048], P('heads'), may hold values from -3 to 3
- w_project: bfloat16 [2048, 512], P('heads'), may hold values from -0.25 to 0.25
- b_project: bfloat16 [512], replicated, may hold values from -3 to 3
- cotangent: bfloat16 [2048, 16, 512], P('heads', 'dp'), may hold values from -6 to 6
Outputs:
- outputs: bfloat16 [2048, 16, 512], P('heads', 'dp')
- grad_inputs: float32 [2048, 16, 512], P('heads', 'dp')
- grad_attn_gain: float32 [512], replicated
- grad_query: float32 [512, 512], P(None, 'heads')
- grad_key: float32 [512, 512], P(None, 'heads')
- grad_value: float32 [512, 512], P(None, 'heads')
- grad_output: float32 [512, 512], P('heads')
- grad_ffn_gain: float32 [512], replicated
- grad_hidden: float32 [512, 2048], P(None, 'heads')
- grad_b_hidden: float32 [2048], P('heads')
- grad_project: float32 [2048, 512], P('heads')
- grad_b_project: float32 [512], replicated
The draws below stay inside these ranges and needn't reach their ends.
Inputs may be any that keep to these rules, and one draw needn't show every extreme that they name: `lengths`: every row has at least 512 valid positions; some row is full and some row has exactly 512.
All inputs are finite; a program needn't handle non-finite values.
Results may differ from the reference program's by a relative error of at most 0.012.
Values may be sent and summed in bfloat16 or wider, within the bound.
A program may use at most 256 MiB of HBM per device.

```python
import jax
import jax.numpy as jnp
from jax import lax

D = 512
HEADS = 8
HD = 64
FF = 2048
BLOCK = 16
ROW_LEN = 2048
ROWS = 16


def draw_lengths(key, part):
    least = ROW_LEN // 4
    drawn = jax.random.randint(jax.random.fold_in(key, 11), (ROWS,), least, ROW_LEN + 1)
    full_at = jax.random.randint(jax.random.fold_in(key, 12), (), 0, ROWS)
    short_at = (full_at + jax.random.randint(jax.random.fold_in(key, 13), (), 1, ROWS)) % ROWS
    places = jnp.arange(ROWS)
    drawn = jnp.where(places == full_at, ROW_LEN, drawn)
    drawn = jnp.where(places == short_at, least, drawn)
    return drawn.astype(jnp.int32)


def steps_of(own_key, extent, pieces, smallest, largest):
    loudness = 1.0
    for axis_at, blocks in pieces:
        steps = jax.random.uniform(jax.random.fold_in(jax.random.fold_in(own_key, 6), axis_at), (blocks,), jnp.float32, smallest / len(pieces), largest / len(pieces))
        loudness = loudness * jnp.repeat(jnp.exp(steps), extent[axis_at] // blocks).reshape((-1,) + (1,) * (len(extent) - 1 - axis_at))
    return loudness


def scatter_about(rng, dims, scale, limit, split=(), held_as=jnp.bfloat16):
    values = scale * jax.random.normal(rng, dims, jnp.float32)
    if split:
        values = values * steps_of(rng, dims, split, -0.22, 0.18)
    return jnp.clip(values, -limit, limit).astype(held_as)


def setup_inputs(seed: int = 0) -> dict:
    splits = jax.random.split(jax.random.key(seed), 14)
    return {
        "inputs": scatter_about(splits[0], (ROW_LEN, ROWS, D), 1.0, 6.0, ((0, 4), (1, 8))),
        "lengths": draw_lengths(jax.random.fold_in(splits[13], 71), 0),
        "attn_gain": jnp.clip(jax.random.uniform(splits[2], (D,), jnp.float32, 0.5, 1.5), 0.5, 1.5).astype(jnp.bfloat16),
        "w_query": scatter_about(splits[3], (D, HEADS * HD), D ** -0.5, 0.25, ((1, 4),)),
        "w_key": scatter_about(splits[4], (D, HEADS * HD), D ** -0.5, 0.25, ((1, 4),)),
        "w_value": scatter_about(splits[5], (D, HEADS * HD), D ** -0.5, 0.25, ((1, 4),)),
        "w_output": scatter_about(splits[6], (HEADS * HD, D), 1.0, 5.0, ((0, 4),)),
        "ffn_gain": jnp.clip(jax.random.uniform(splits[7], (D,), jnp.float32, 0.5, 1.5), 0.5, 1.5).astype(jnp.bfloat16),
        "w_hidden": scatter_about(splits[8], (D, FF), D ** -0.5, 0.25, ((1, 4),)),
        "b_hidden": scatter_about(splits[9], (FF,), 0.7, 3.0, ((0, 4),)),
        "w_project": scatter_about(splits[10], (FF, D), (FF // 4) ** -0.5, 0.25, ((0, 4),)),
        "b_project": scatter_about(splits[11], (D,), 0.5, 3.0),
        "cotangent": scatter_about(splits[12], (ROW_LEN, ROWS, D), 1.0, 6.0, ((0, 4), (1, 8))),
    }


EPS = 1e-05
HIGH = lax.Precision.HIGHEST

@jax.custom_vjp
def low(v):
    return lax.optimization_barrier(v.astype(jnp.bfloat16)).astype(jnp.float32)

@jax.custom_vjp
def low_back(v):
    return v

def low_keep(v):
    return (low(v), None)

def low_pass(kept, grad):
    return (grad,)

def back_keep(v):
    return (v, None)

def back_low(kept, grad):
    return (low(grad),)
low.defvjp(low_keep, low_pass)
low_back.defvjp(back_keep, back_low)

def layer_norm(values, gain):
    center = values - lax.optimization_barrier(jnp.mean(values, axis=-1, keepdims=True))
    spread = lax.optimization_barrier(jnp.mean(center * center, axis=-1, keepdims=True))
    return center * lax.rsqrt(spread + EPS) * gain

def pair_sum(values):
    return values.reshape((values.shape[0] // 2, 2) + values.shape[1:]).sum(axis=1)

def sibling(blocks):
    paired = blocks.reshape((blocks.shape[0] // 2, 2) + blocks.shape[1:])
    return paired[:, ::-1].reshape(blocks.shape)

def level_attend(queries, key_rows, value_rows, counts, with_diag):
    blocks = queries.shape[0] // BLOCK
    query_blocks = queries.reshape((blocks, BLOCK) + queries.shape[1:])
    key_blocks = key_rows.reshape((blocks, BLOCK) + key_rows.shape[1:])
    value_blocks = value_rows.reshape((blocks, BLOCK) + value_rows.shape[1:])
    count_blocks = counts.reshape((blocks, BLOCK) + counts.shape[1:])
    key_near = sibling(key_blocks)
    value_near = sibling(value_blocks)
    count_near = sibling(count_blocks)
    if with_diag:
        key_near = jnp.concatenate([key_blocks, key_near], axis=1)
        value_near = jnp.concatenate([value_blocks, value_near], axis=1)
        count_near = jnp.concatenate([count_blocks, count_near], axis=1)
    scores = jnp.einsum('nibhe,njbhe->nbhij', query_blocks, key_near, precision=HIGH) * HD ** (-0.5)
    weights = jnp.exp(scores)
    numerator = jnp.einsum('nbhij,njbhe->nibhe', weights, value_near, precision=HIGH)
    denominator = jnp.einsum('nbhij,njb->nibh', weights, count_near, precision=HIGH)
    return (numerator.reshape(queries.shape), denominator.reshape(queries.shape[:3]))

def hier_attention(queries, key_rows, value_rows, valid_mask):
    depths = (queries.shape[0] // BLOCK).bit_length() - 1
    coarse_q = queries
    coarse_k = key_rows
    coarse_v = value_rows * valid_mask[:, :, None, None]
    counts = valid_mask
    numerators = []
    denominators = []
    for depth_idx in range(depths):
        if depth_idx > 0:
            coarse_q = 0.5 * pair_sum(coarse_q)
            coarse_k = 0.5 * pair_sum(coarse_k)
            coarse_v = pair_sum(coarse_v)
            counts = pair_sum(counts)
        level_num, level_den = level_attend(coarse_q, coarse_k, coarse_v, counts, depth_idx == 0)
        numerators.append(level_num)
        denominators.append(level_den)
    acc_numer = numerators[-1]
    acc_denom = denominators[-1]
    for depth_idx in range(depths - 2, -1, -1):
        acc_numer = numerators[depth_idx] + jnp.repeat(acc_numer, 2, axis=0)
        acc_denom = denominators[depth_idx] + jnp.repeat(acc_denom, 2, axis=0)
    return acc_numer / acc_denom[..., None]

def block_forward(inputs, params, valid_mask):
    attn_gain, w_query, w_key, w_value, w_output, ffn_gain, w_hidden, b_hidden, w_project, b_project = params
    length = inputs.shape[0]
    batch_rows = inputs.shape[1]
    normed = low(layer_norm(inputs, attn_gain))

    def project(weight):
        projected = jnp.einsum('lbd,de->lbe', normed, weight, precision=HIGH)
        return low(low_back(projected)).reshape(length, batch_rows, HEADS, HD)
    attended = hier_attention(project(w_query), project(w_key), project(w_value), valid_mask)
    mixed = low(low_back(attended.reshape(length, batch_rows, HEADS * HD)))
    attn_branch = jnp.einsum('lbe,ed->lbd', mixed, w_output, precision=HIGH)
    residual = inputs + low_back(attn_branch)
    normed_ffn = low(layer_norm(residual, ffn_gain))
    pre = low_back(jnp.einsum('lbd,df->lbf', normed_ffn, w_hidden, precision=HIGH) + b_hidden)
    act = low(jax.nn.gelu(pre, approximate=True))
    ffn_branch = jnp.einsum('lbf,fd->lbd', act, w_project, precision=HIGH) + b_project
    return residual + low_back(ffn_branch)

def reference(inputs, lengths, attn_gain, w_query, w_key, w_value, w_output, ffn_gain, w_hidden, b_hidden, w_project, b_project, cotangent):
    group_rows = min(ROWS, max(1, 4096 // ROW_LEN))
    groups = ROWS // group_rows
    positions = jnp.arange(ROW_LEN, dtype=jnp.int32)
    valid_mask = (positions[:, None] < lengths[None, :].astype(jnp.int32)).astype(jnp.float32)
    params = tuple((param.astype(jnp.float32) for param in (attn_gain, w_query, w_key, w_value, w_output, ffn_gain, w_hidden, b_hidden, w_project, b_project)))
    masked_cot = cotangent.astype(jnp.float32) * valid_mask[:, :, None]

    def regroup(values):
        return jnp.swapaxes(values.reshape((ROW_LEN, groups, group_rows) + values.shape[2:]), 0, 1)

    def one_group(totals, item):
        group_inputs, group_cot, group_mask = item

        def forward_group(group_values, group_params):
            return block_forward(group_values, group_params, group_mask)
        group_out, pullback = jax.vjp(forward_group, group_inputs, params)
        grad_group, grad_params = pullback(group_cot)
        totals = jax.tree.map(lambda first, second: first + second, totals, grad_params)
        return (totals, (group_out, grad_group))
    zeros = jax.tree.map(jnp.zeros_like, params)
    grads, (outs_all, grads_in) = lax.scan(one_group, zeros, (regroup(inputs.astype(jnp.float32)), regroup(masked_cot), regroup(valid_mask)))
    outputs = jnp.swapaxes(outs_all, 0, 1).reshape(ROW_LEN, ROWS, D).astype(jnp.bfloat16)
    grad_inputs = jnp.swapaxes(grads_in, 0, 1).reshape(ROW_LEN, ROWS, D)
    return (outputs, grad_inputs, grads[0], grads[1], grads[2], grads[3], grads[4], grads[5], grads[6], grads[7], grads[8], grads[9])
```

```python
import functools

import jax
import jax.numpy as jnp
from jax import lax
from jax.experimental import pallas as pl
from jax.experimental.pallas import tpu as pltpu
from jax.sharding import PartitionSpec as P

HD = 64
BLOCK = 16
EPS = 1e-05
SEG = 512
LOCAL = 5
f32 = jnp.float32
bf16 = jnp.bfloat16
NEG = -1e30
VMEM_LIMIT = 66 * 1024 * 1024 - 2 * 1024 * 1024


def nn(a, b):
    return lax.dot_general(a, b, (((1,), (0,)), ((), ())), preferred_element_type=f32)


def nt(a, b):
    return lax.dot_general(a, b, (((1,), (1,)), ((), ())), preferred_element_type=f32)


def tn(a, b):
    return lax.dot_general(a, b, (((0,), (0,)), ((), ())), preferred_element_type=f32)


def iota(shape, dim):
    return lax.broadcasted_iota(jnp.int32, shape, dim)


def level_of(row):
    level = jnp.ones_like(row)
    start = jnp.zeros_like(row)
    edge, size = 256, 256
    for _ in range(7):
        past = row >= edge
        level = level + past.astype(jnp.int32)
        start = jnp.where(past, edge, start)
        size //= 2
        edge += size
    return level, row - start


def pool_matrices():
    row, pos = iota((SEG, SEG), 0), iota((SEG, SEG), 1)
    level, index = level_of(row)
    hit = (lax.shift_right_logical(pos, level) == index) & (row < 508)
    mean = lax.shift_left(jnp.ones_like(level), 8 - level).astype(f32) * (1.0 / 256.0)
    m_sum = jnp.where(hit, 1.0, 0.0)
    m_mean = jnp.where(hit, mean, 0.0)
    return m_sum.astype(bf16), m_mean.astype(bf16), m_sum.T.astype(bf16), m_mean.T.astype(bf16)


def norm_parts(values):
    center = values - jnp.mean(values, axis=-1, keepdims=True)
    spread = jnp.mean(center * center, axis=-1, keepdims=True)
    inv = lax.rsqrt(spread + EPS)
    return center * inv, inv


def norm_back(grad, gain, hat, inv):
    t = grad * gain
    return (t - jnp.mean(t, axis=-1, keepdims=True) - hat * jnp.mean(t * hat, axis=-1, keepdims=True)) * inv


def params(**extra):
    return pltpu.CompilerParams(vmem_limit_bytes=VMEM_LIMIT, **extra)


def vmem_specs(count):
    return [pl.BlockSpec(memory_space=pltpu.VMEM)] * count


def project_kernel(info, x, gain, w_qkv, m_sum, m_mean, normed, q_all, k_all, v_all, ex):
    rows = x.shape[0]
    for r in range(rows):
        for c in range(2):
            at = c * 256
            hat, _ = norm_parts(x[r, at : at + 256, :].astype(f32))
            nb = (hat * gain[...]).astype(bf16)
            normed[r, at : at + 256, :] = nb
            q = nt(nb, w_qkv[0:SEG, :]).astype(bf16)
            k = nt(nb, w_qkv[SEG : 2 * SEG, :]).astype(bf16)
            v = nt(nb, w_qkv[2 * SEG :, :])
            pos = iota((256, SEG), 0) + (at + info[rows])
            v = jnp.where(pos < info[r], v, 0.0).astype(bf16)
            q_all[r, at : at + 256, :] = q * jnp.asarray(HD**-0.5, bf16)
            k_all[r, at : at + 256, :] = k
            v_all[r, at : at + 256, :] = v
        q_all[r, SEG:, :] = nn(m_mean[...], q_all[r, :SEG, :]).astype(bf16)
        k_all[r, SEG:, :] = nn(m_mean[...], k_all[r, :SEG, :]).astype(bf16)
        v_all[r, SEG:, :] = nn(m_sum[...], v_all[r, :SEG, :]).astype(bf16)
        ex[0, r] = k_all[r, 2 * SEG - 32 :, :]
        ex[1, r] = v_all[r, 2 * SEG - 32 :, :]


def fill_bias(bias, bias7):
    q = iota((128, 256), 0)
    k = iota((128, 256), 1) & 127
    bias[0] = jnp.where((q >> 5) == (k >> 5), 0.0, NEG)
    bias[1] = jnp.where(((q >> 4) ^ (k >> 4)) == 1, 0.0, NEG)
    wide = bias7.shape[1] // 2
    q = iota((128, 2 * wide), 0)
    k = iota((128, 2 * wide), 1)
    k = jnp.where(k >= wide, k - wide, k)
    ok = (((q >> 4) ^ (k >> 4)) == 1) & (q < 96) & (k < 96)
    ok = ok | ((q >= 96) & (q < 112) & (k >= 96) & (k < 112))
    ok = ok | ((q >= 112) & (q < 120) & (k >= 112) & (k < 128))
    ok = ok | ((q >= 120) & (q < 124) & (k >= 128) & (k < 144))
    bias7[...] = jnp.where(ok, 0.0, NEG)


def fill_bias_t(bias, bias7):
    k = iota((256, 128), 0) & 127
    q = iota((256, 128), 1)
    bias[0] = jnp.where((q >> 5) == (k >> 5), 0.0, NEG)
    bias[1] = jnp.where(((q >> 4) ^ (k >> 4)) == 1, 0.0, NEG)
    wide = bias7.shape[0] // 2
    k = iota((2 * wide, 128), 0)
    k = jnp.where(k >= wide, k - wide, k)
    q = iota((2 * wide, 128), 1)
    ok = (((q >> 4) ^ (k >> 4)) == 1) & (q < 96) & (k < 96)
    ok = ok | ((q >= 96) & (q < 112) & (k >= 96) & (k < 112))
    ok = ok | ((q >= 112) & (q < 120) & (k >= 112) & (k < 128))
    ok = ok | ((q >= 120) & (q < 124) & (k >= 128) & (k < 144))
    bias7[...] = jnp.where(ok, 0.0, NEG)


def fill_counts(info, rows, remote, counts, counts_far):
    pos0 = info[rows]
    me = info[rows + 1]
    for r in range(rows):
        length = info[r]
        at = iota((SEG, 128), 0)
        counts[r, :SEG, :] = jnp.where(at + pos0 < length, 1.0, 0.0).astype(bf16)
        level, index = level_of(at)
        size = lax.shift_left(jnp.ones_like(level), level)
        start = pos0 + index * size
        counts[r, SEG:, :] = jnp.clip(length - start, 0, size).astype(f32).astype(bf16)
        for m in range(remote):
            size_m = 1 << (LOCAL + m)
            group = (me >> m) ^ 1
            start = group * ((1 << m) * SEG) + iota((16, 128), 0) * size_m
            counts_far[r, 16 * m : 16 * m + 16, :] = jnp.clip(length - start, 0, size_m).astype(f32).astype(bf16)


def pair_split(values, low):
    zero = jnp.zeros_like(values)
    return jnp.concatenate([jnp.where(low, values, zero), jnp.where(low, zero, values)], axis=0)


def last_rows(local, far, wide):
    parts = [local, far]
    rest = wide - local.shape[0] - far.shape[0]
    if rest:
        parts.append(jnp.zeros((rest, local.shape[1]), local.dtype))
    return jnp.concatenate(parts, axis=0)


def key_tile(t, r, lanes, k_all, v_all, counts, k_far, v_far, counts_far, wide):
    if t < 7:
        at = slice(128 * t, 128 * t + 128)
        return k_all[r, at, lanes], v_all[r, at, lanes], counts[r, at, :]
    at = slice(896, 992)
    return (
        last_rows(k_all[r, at, lanes], k_far[r, :, lanes], wide),
        last_rows(v_all[r, at, lanes], v_far[r, :, lanes], wide),
        last_rows(counts[r, at, :], counts_far[r], wide),
    )


def bias_of(t, bias, bias7):
    if t < 4:
        return bias[0]
    if t < 7:
        return bias[1]
    return bias7[...]


def attend_kernel(
    info, q_all, k_all, v_all, k_far, v_far, u_sum, mixed, rden, counts, counts_far, bias, bias7, pyr
):
    rows = q_all.shape[0]
    remote = k_far.shape[1] // 16
    wide = bias7.shape[1] // 2
    fill_bias(bias, bias7)
    fill_counts(info, rows, remote, counts, counts_far)
    low = iota((128, 128), 1) < HD
    low7 = iota((wide, 128), 1) < HD

    def step(it, _):
        r = it // 4
        lanes = pl.ds(pl.multiple_of((it % 4) * 128, 128), 128)
        base = []
        for t in range(8):
            q = q_all[r, 128 * t : 128 * t + 128, lanes]
            k, v, c = key_tile(t, r, lanes, k_all, v_all, counts, k_far, v_far, counts_far, wide)
            lm = low if t < 7 else low7
            score = nt(q, pair_split(k, lm)) + bias_of(t, bias, bias7)
            weight = jnp.exp(score).astype(bf16)
            both = nn(weight, jnp.concatenate([pair_split(v, lm), pair_split(c, lm)], axis=1))
            if t < 4:
                base.append(both)
            else:
                pyr[128 * (t - 4) : 128 * (t - 4) + 128, :] = both.astype(bf16)
        for t in range(4):
            total = base[t] + nn(u_sum[128 * t : 128 * t + 128, :], pyr[...])
            inv = 1.0 / total[:, 128:]
            mixed[r, 128 * t : 128 * t + 128, lanes] = (total[:, :128] * inv).astype(bf16)
            rden[r, 128 * t : 128 * t + 128, lanes] = inv
        return 0

    lax.fori_loop(0, rows * 4, step, 0)


def ffn_kernel(
    info, x, mixed, cot, w_out, w_hid, w_proj, b_hid, b_proj, gain,
    out, g_res, g_mixed, gw_proj, gw_hid, gw_out, gb_hid, small,
    res, hat, inv_s, n2, gout, ffn, gn2, act_s, gpre_s,
):
    rows = x.shape[0]
    chunk = 256
    units = 512
    steps = SEG // chunk
    for r in range(rows):
        for c in range(steps):
            at = slice(c * chunk, c * chunk + chunk)
            to = slice(r * SEG + c * chunk, r * SEG + c * chunk + chunk)
            value = x[r, at, :].astype(f32) + nn(mixed[r, at, :], w_out[...])
            res[to, :] = value
            h, s = norm_parts(value)
            hat[to, :] = h
            inv_s[to, :] = jnp.broadcast_to(s, (chunk, 128))
            n2[to, :] = (h * gain[...]).astype(bf16)
            pos = iota((chunk, SEG), 0) + (c * chunk + info[rows])
            gout[to, :] = jnp.where(pos < info[r], cot[r, at, :].astype(f32), 0.0).astype(bf16)
    gb_hid[...] = jnp.zeros_like(gb_hid)

    def unit_step(f, _):
        us = pl.ds(pl.multiple_of(f * units, units), units)

        def token_step(c, _):
            to = pl.ds(pl.multiple_of(c * chunk, chunk), chunk)
            pre = nt(n2[to, :], w_hid[us, :]) + b_hid[:, us]
            k0 = 0.7978845608028654
            sq = pre * pre
            t = jnp.tanh(k0 * pre * (1.0 + 0.044715 * sq))
            half = 0.5 + 0.5 * t
            act = (pre * half).astype(bf16)
            slope = half + 0.5 * pre * (1.0 - t * t) * (k0 + (3.0 * 0.044715 * k0) * sq)
            gpre = nt(gout[to, :], w_proj[us, :]) * slope
            gpre_b = gpre.astype(bf16)
            act_s[to, :] = act
            gpre_s[to, :] = gpre_b
            part = gpre_b.astype(f32).reshape(chunk // 8, 8, units).sum(axis=0)
            gb_hid[:, us] = gb_hid[:, us] + part
            add_f = nn(act, w_proj[us, :])
            add_g = nn(gpre_b, w_hid[us, :])

            @pl.when(f == 0)
            def _():
                ffn[to, :] = add_f
                gn2[to, :] = add_g

            @pl.when(f > 0)
            def _():
                ffn[to, :] = ffn[to, :] + add_f
                gn2[to, :] = gn2[to, :] + add_g

            return 0

        lax.fori_loop(0, rows * steps, token_step, 0)
        gw_proj[us, :] = tn(act_s[...], gout[...])
        gw_hid[us, :] = tn(gpre_s[...], n2[...])
        return 0

    lax.fori_loop(0, w_hid.shape[0] // units, unit_step, 0)

    sum_gain = jnp.zeros((8, SEG), f32)
    sum_out = jnp.zeros((8, SEG), f32)
    for r in range(rows):
        for c in range(steps):
            at = slice(c * chunk, c * chunk + chunk)
            to = slice(r * SEG + c * chunk, r * SEG + c * chunk + chunk)
            out[r, at, :] = (res[to, :] + ffn[to, :] + b_proj[...]).astype(bf16)
            go = gout[to, :].astype(f32)
            h = hat[to, :]
            g = gn2[to, :]
            sum_gain = sum_gain + (g * h).reshape(chunk // 8, 8, SEG).sum(axis=0)
            sum_out = sum_out + go.reshape(chunk // 8, 8, SEG).sum(axis=0)
            inv = inv_s[to, :][:, :1]
            gr = go + norm_back(g, gain[...], h, inv)
            g_res[r, at, :] = gr
            grb = gr.astype(bf16)
            n2[to, :] = grb
            g_mixed[r, at, :] = nt(grb, w_out[...]).astype(bf16)
    small[0] = sum_gain
    small[1] = sum_out
    acc = jnp.zeros((SEG, SEG), f32)
    for r in range(rows):
        acc = acc + tn(mixed[r], n2[r * SEG : r * SEG + SEG, :])
    gw_out[...] = acc


def attend_back_kernel(
    info, q_all, k_all, v_all, k_far, v_far, mixed, rden, g_mixed, m_sum, u_sum, u_mean,
    g_q, g_k, g_v, gk_far, gv_far,
    counts, counts_far, bias, bias7, bias_t, bias7_t, grad, gp_q, gp_k, gp_v,
):
    rows = q_all.shape[0]
    remote = k_far.shape[1] // 16
    wide = bias7.shape[1] // 2
    fill_bias(bias, bias7)
    fill_bias_t(bias_t, bias7_t)
    fill_counts(info, rows, remote, counts, counts_far)
    low = iota((128, 128), 1) < HD
    low7 = iota((wide, 128), 1) < HD

    def step(it, _):
        r = it // 4
        lanes = pl.ds(pl.multiple_of((it % 4) * 128, 128), 128)
        gnum = g_mixed[r, :, lanes].astype(f32) * rden[r, :, lanes]
        gden = -gnum * mixed[r, :, lanes].astype(f32)
        grad[:SEG, :] = jnp.concatenate([gnum, gden], axis=1).astype(bf16)
        grad[SEG:, :] = nn(m_sum[...], grad[:SEG, :]).astype(bf16)
        base_q, base_k, base_v = [], [], []
        for t in range(8):
            at = slice(128 * t, 128 * t + 128)
            q = q_all[r, at, lanes]
            k, v, c = key_tile(t, r, lanes, k_all, v_all, counts, k_far, v_far, counts_far, wide)
            lm = low if t < 7 else low7
            n_keys = 128 if t < 7 else wide
            g = grad[at, :]
            kk = pair_split(k, lm)
            vv = jnp.concatenate([pair_split(v, lm), pair_split(c, lm)], axis=1)
            weight = jnp.exp(nt(q, kk) + bias_of(t, bias, bias7))
            gs = (weight * nt(g, vv)).astype(bf16)
            gq = nn(gs, kk)
            weight_t = jnp.exp(nt(kk, q) + bias_of(t, bias_t, bias7_t))
            gs_t = (weight_t * nt(vv, g)).astype(bf16)
            gk = nn(gs_t, q)
            gv = nn(weight_t.astype(bf16), g[:, :128])
            gk = jnp.where(lm, gk[:n_keys], gk[n_keys:])
            gv = jnp.where(lm, gv[:n_keys], gv[n_keys:])
            if t < 4:
                base_q.append(gq)
                base_k.append(gk)
                base_v.append(gv)
            else:
                to = slice(128 * (t - 4), 128 * (t - 4) + 128)
                gp_q[to, :] = gq.astype(bf16)
                if t < 7:
                    gp_k[to, :] = gk.astype(bf16)
                    gp_v[to, :] = gv.astype(bf16)
                else:
                    gp_k[384:480, :] = gk[:96].astype(bf16)
                    gp_v[384:480, :] = gv[:96].astype(bf16)
                    gp_k[480:, :] = jnp.zeros((32, 128), bf16)
                    gp_v[480:, :] = jnp.zeros((32, 128), bf16)
                    gk_far[r, :, lanes] = gk[96 : 96 + 16 * remote].astype(bf16)
                    gv_far[r, :, lanes] = gv[96 : 96 + 16 * remote].astype(bf16)
        for t in range(4):
            at = slice(128 * t, 128 * t + 128)
            gq = (base_q[t] + nn(u_mean[at, :], gp_q[...])) * (HD**-0.5)
            g_q[r, at, lanes] = gq.astype(bf16)
            g_k[r, at, lanes] = base_k[t] + nn(u_mean[at, :], gp_k[...])
            g_v[r, at, lanes] = base_v[t] + nn(u_sum[at, :], gp_v[...])
        return 0

    lax.fori_loop(0, rows * 4, step, 0)


def finish_kernel(
    info, x, normed, gain, w_qkv, g_q, g_k, g_v, gk_in, gv_in, u_sum, u_mean, g_res,
    g_in, gw_qkv, small, gkb, gvb,
):
    rows = x.shape[0]
    chunk = 256
    sum_gain = jnp.zeros((8, SEG), f32)
    for r in range(rows):
        for c in range(SEG // chunk):
            at = slice(c * chunk, c * chunk + chunk)
            gk = g_k[r, at, :] + nn(u_mean[at, 480:], gk_in[r])
            gv = g_v[r, at, :] + nn(u_sum[at, 480:], gv_in[r])
            pos = iota((chunk, SEG), 0) + (c * chunk + info[rows])
            gv = jnp.where(pos < info[r], gv, 0.0)
            gkb[r, at, :] = gk.astype(bf16)
            gvb[r, at, :] = gv.astype(bf16)
            gn = nn(g_q[r, at, :], w_qkv[:SEG, :])
            gn = gn + nn(gkb[r, at, :], w_qkv[SEG : 2 * SEG, :])
            gn = gn + nn(gvb[r, at, :], w_qkv[2 * SEG :, :])
            h, inv = norm_parts(x[r, at, :].astype(f32))
            sum_gain = sum_gain + (gn * h).reshape(chunk // 8, 8, SEG).sum(axis=0)
            g_in[r, at, :] = g_res[r, at, :] + norm_back(gn, gain[...], h, inv)
    small[...] = sum_gain
    for part, src in enumerate((g_q, gkb, gvb)):
        acc = tn(src[0], normed[0])
        for r in range(1, rows):
            acc = acc + tn(src[r], normed[r])
        gw_qkv[part * SEG : part * SEG + SEG, :] = acc


def sds(shape, dtype):
    return jax.ShapeDtypeStruct(shape, dtype)


def body(
    inputs, lengths, attn_gain, w_query, w_key, w_value, w_output, ffn_gain, w_hidden, b_hidden,
    w_project, b_project, cotangent,
):
    seg, rows = inputs.shape[0], inputs.shape[1]
    assert seg == SEG and inputs.shape[2] == SEG
    heads = lax.axis_size("heads")
    dps = lax.axis_size("dp")
    remote = heads.bit_length() - 1
    me = lax.axis_index("heads")
    dp = lax.axis_index("dp")
    hw = w_query.shape[1]
    units = w_hidden.shape[1]
    info = jnp.concatenate([lengths, (me * SEG)[None], me[None]]).astype(jnp.int32)

    def gather(shard):
        piece = shard.reshape((dps, shard.shape[0] // dps, SEG))
        piece = lax.dynamic_index_in_dim(piece, dp, 0, keepdims=False)
        full = lax.all_gather(piece, "heads", axis=0)
        full = lax.all_gather(full, "dp", axis=1)
        return full.reshape((-1, SEG))

    local_qkv = jnp.stack([w_query.T, w_key.T, w_value.T])
    piece = local_qkv.reshape(3, dps, hw // dps, SEG)
    piece = lax.dynamic_index_in_dim(piece, dp, 1, keepdims=False)
    full = lax.all_gather(piece, "heads", axis=1)
    full = lax.all_gather(full, "dp", axis=2)
    w_qkv = full.reshape(3 * SEG, SEG)
    w_out = gather(w_output)
    w_hid = gather(w_hidden.T)
    w_proj = gather(w_project)
    b_hid = lax.all_gather(b_hidden.astype(f32), "heads", axis=0, tiled=True)[None, :]

    x = inputs.transpose(1, 0, 2)
    cot = cotangent.transpose(1, 0, 2)
    gain1 = attn_gain.astype(f32)[None, :]
    gain2 = ffn_gain.astype(f32)[None, :]
    b_proj = b_project.astype(f32)[None, :]
    m_sum, m_mean, u_sum, u_mean = pool_matrices()
    smem = pl.BlockSpec(memory_space=pltpu.SMEM)
    vec = pl.BlockSpec(memory_space=pltpu.VMEM)

    def call(kernel, outs, scratch, *args):
        return pl.pallas_call(
            kernel,
            out_shape=outs,
            in_specs=[smem] + [vec] * (len(args) - 1),
            out_specs=[vec] * len(outs),
            scratch_shapes=scratch,
            compiler_params=params(),
        )(*args)

    tok = (rows, SEG, SEG)
    pyr = (rows, 2 * SEG, SEG)
    normed, q_all, k_all, v_all, ex = call(
        project_kernel,
        [sds(tok, bf16), sds(pyr, bf16), sds(pyr, bf16), sds(pyr, bf16), sds((2, rows, 32, SEG), bf16)],
        [],
        info, x, gain1, w_qkv, m_sum, m_mean,
    )
    got = lax.all_gather(ex, "heads", axis=0)
    far = []
    for m in range(remote):
        group = (me >> m) ^ 1
        part = lax.dynamic_slice_in_dim(got, group << m, 1 << m, 0)
        first = 32 - (32 >> m)
        part = part[:, :, :, first : first + (16 >> m), :]
        far.append(part.transpose(1, 2, 0, 3, 4).reshape(2, rows, 16, SEG))
    far = jnp.concatenate(far, axis=2)
    k_far, v_far = far[0], far[1]

    wide = 128 * ((96 + 16 * remote + 127) // 128)
    att_scratch = [
        pltpu.VMEM((rows, 2 * SEG, 128), bf16),
        pltpu.VMEM((rows, 16 * remote, 128), bf16),
        pltpu.VMEM((2, 128, 256), f32),
        pltpu.VMEM((128, 2 * wide), f32),
    ]
    mixed, rden = call(
        attend_kernel,
        [sds(tok, bf16), sds(tok, f32)],
        att_scratch + [pltpu.VMEM((SEG, 256), bf16)],
        info, q_all, k_all, v_all, k_far, v_far, u_sum,
    )
    flat = (rows * SEG, SEG)
    ff = w_hid.shape[0]
    out, g_res, g_mixed, gw_proj, gw_hid, gw_out, gb_hid, small2 = call(
        ffn_kernel,
        [
            sds(tok, bf16), sds(tok, f32), sds(tok, bf16), sds((ff, SEG), f32), sds((ff, SEG), f32),
            sds((SEG, SEG), f32), sds((8, ff), f32), sds((2, 8, SEG), f32),
        ],
        [
            pltpu.VMEM(flat, f32), pltpu.VMEM(flat, f32), pltpu.VMEM((rows * SEG, 128), f32),
            pltpu.VMEM(flat, bf16), pltpu.VMEM(flat, bf16), pltpu.VMEM(flat, f32), pltpu.VMEM(flat, f32),
            pltpu.VMEM((rows * SEG, 512), bf16), pltpu.VMEM((rows * SEG, 512), bf16),
        ],
        info, x, mixed, cot, w_out, w_hid, w_proj, b_hid, b_proj, gain2,
    )

    def reduce(grad):
        mine = lax.psum_scatter(grad, ("heads", "dp"), scatter_dimension=0, tiled=True)
        return lax.all_gather(mine, "dp", axis=0, tiled=True)

    grad_ffn = reduce(jnp.stack([gw_hid, gw_proj], axis=0).reshape(2, heads, dps, units // dps, SEG)
                      .transpose(1, 2, 0, 3, 4).reshape(-1, SEG))
    grad_ffn = grad_ffn.reshape(dps, 2, units // dps, SEG).transpose(1, 0, 2, 3).reshape(2, units, SEG)

    g_q, g_k, g_v, gk_far, gv_far = call(
        attend_back_kernel,
        [
            sds(tok, bf16), sds(tok, f32), sds(tok, f32),
            sds((rows, 16 * remote, SEG), bf16), sds((rows, 16 * remote, SEG), bf16),
        ],
        att_scratch + [
            pltpu.VMEM((2, 256, 128), f32), pltpu.VMEM((2 * wide, 128), f32),
            pltpu.VMEM((2 * SEG, 256), bf16),
            pltpu.VMEM((SEG, 128), bf16), pltpu.VMEM((SEG, 128), bf16), pltpu.VMEM((SEG, 128), bf16),
        ],
        info, q_all, k_all, v_all, k_far, v_far, mixed, rden, g_mixed, m_sum, u_sum, u_mean,
    )
    back = lax.all_gather(jnp.stack([gk_far, gv_far]), "heads", axis=0)
    near = []
    for m in range(remote):
        group = (me >> m) ^ 1
        part = lax.dynamic_slice_in_dim(back, group << m, 1 << m, 0)
        part = part[:, :, :, 16 * m : 16 * m + 16, :].astype(f32).sum(axis=0)
        count = 16 >> m
        near.append(lax.dynamic_slice_in_dim(part, (me & ((1 << m) - 1)) * count, count, 2))
    pad = 32 - sum(p.shape[2] for p in near)
    near = jnp.concatenate(near + [jnp.zeros((2, rows, pad, SEG), f32)], axis=2).astype(bf16)

    g_in, gw_qkv, small1 = call(
        finish_kernel,
        [sds(tok, f32), sds((3 * SEG, SEG), f32), sds((8, SEG), f32)],
        [pltpu.VMEM(tok, bf16), pltpu.VMEM(tok, bf16)],
        info, x, normed, gain1, w_qkv, g_q, g_k, g_v, near[0], near[1], u_sum, u_mean, g_res,
    )
    every = jnp.concatenate([gw_qkv, gw_out], axis=0).reshape(4, heads, dps, hw // dps, SEG)
    grad_att = reduce(every.transpose(1, 2, 0, 3, 4).reshape(-1, SEG))
    grad_att = grad_att.reshape(dps, 4, hw // dps, SEG).transpose(1, 0, 2, 3).reshape(4, hw, SEG)

    tiny = jnp.concatenate([small1.sum(0), small2.sum(1).reshape(-1), gb_hid.sum(0)])
    tiny = lax.psum(tiny, ("dp", "heads"))
    gb = lax.dynamic_slice_in_dim(tiny[3 * SEG :], me * units, units, 0)
    return (
        out.transpose(1, 0, 2),
        g_in.transpose(1, 0, 2),
        tiny[:SEG],
        grad_att[0].T,
        grad_att[1].T,
        grad_att[2].T,
        grad_att[3],
        tiny[SEG : 2 * SEG],
        grad_ffn[0].T,
        gb,
        grad_ffn[1],
        tiny[2 * SEG : 3 * SEG],
    )


def solution(mesh):
    rows = P("heads", "dp", None)
    cols, flat, tall = P(None, "heads"), P("heads"), P("heads", None)
    return jax.shard_map(
        body,
        mesh=mesh,
        in_specs=(rows, P("dp"), P(), cols, cols, cols, tall, P(), cols, flat, tall, P(), rows),
        out_specs=(rows, rows, P(), cols, cols, cols, tall, P(), cols, flat, tall, P()),
        check_vma=False,
    )
```

```python
import functools

import jax
import jax.numpy as jnp
from jax import lax
from jax.experimental import pallas as pl
from jax.experimental.pallas import tpu as pltpu
from jax.sharding import PartitionSpec as P

HD = 64
BLOCK = 16
EPS = 1e-05
SEG = 512
LOCAL = 5
f32 = jnp.float32
bf16 = jnp.bfloat16
NEG = -1e30
VMEM_LIMIT = 66 * 1024 * 1024 - 2 * 1024 * 1024


def nn(a, b):
    return lax.dot_general(a, b, (((1,), (0,)), ((), ())), preferred_element_type=f32)


def nt(a, b):
    return lax.dot_general(a, b, (((1,), (1,)), ((), ())), preferred_element_type=f32)


def tn(a, b):
    return lax.dot_general(a, b, (((0,), (0,)), ((), ())), preferred_element_type=f32)


def iota(shape, dim):
    return lax.broadcasted_iota(jnp.int32, shape, dim)


def level_of(row):
    level = jnp.ones_like(row)
    start = jnp.zeros_like(row)
    edge, size = 256, 256
    for _ in range(7):
        past = row >= edge
        level = level + past.astype(jnp.int32)
        start = jnp.where(past, edge, start)
        size //= 2
        edge += size
    return level, row - start


def pool_matrix(transposed, mean):
    row, pos = iota((SEG, SEG), int(transposed)), iota((SEG, SEG), 1 - int(transposed))
    level, index = level_of(row)
    hit = (lax.shift_right_logical(pos, level) == index) & (row < 508)
    part = 1.0
    if mean:
        part = lax.shift_left(jnp.ones_like(level), 8 - level).astype(f32) * (1.0 / 256.0)
    return jnp.where(hit, part, 0.0).astype(bf16)


def pool_matrices():
    return tuple(pool_matrix(*kind) for kind in ((False, False), (False, True), (True, False), (True, True)))


def norm_parts(values):
    center = values - jnp.mean(values, axis=-1, keepdims=True)
    spread = jnp.mean(center * center, axis=-1, keepdims=True)
    inv = lax.rsqrt(spread + EPS)
    return center * inv, inv


def norm_back(grad, gain, hat, inv):
    t = grad * gain
    return (t - jnp.mean(t, axis=-1, keepdims=True) - hat * jnp.mean(t * hat, axis=-1, keepdims=True)) * inv


def params(**extra):
    return pltpu.CompilerParams(vmem_limit_bytes=VMEM_LIMIT, **extra)


def vmem_specs(count):
    return [pl.BlockSpec(memory_space=pltpu.VMEM)] * count


def norm_phase(x, gain, normed):
    for r in range(x.shape[0]):
        for c in range(2):
            at = slice(c * 256, c * 256 + 256)
            hat, _ = norm_parts(x[r, at, :].astype(f32))
            normed[r, at, :] = (hat * gain[...]).astype(bf16)


def project_phase(info, r, normed, weight, m_sum, m_mean, q_all, k_all, v_all):
    rows = normed.shape[0]
    for c in range(2):
        at = slice(c * 256, c * 256 + 256)
        nb = normed[r, at, :]
        q = nt(nb, weight(0)).astype(bf16)
        q_all[r, at, :] = q * jnp.asarray(HD**-0.5, bf16)
        k_all[r, at, :] = nt(nb, weight(1)).astype(bf16)
        pos = iota((256, SEG), 0) + (c * 256 + info[rows])
        v_all[r, at, :] = jnp.where(pos < info[r], nt(nb, weight(2)), 0.0).astype(bf16)
    q_all[r, SEG:, :] = nn(m_mean[...], q_all[r, :SEG, :]).astype(bf16)
    k_all[r, SEG:, :] = nn(m_mean[...], k_all[r, :SEG, :]).astype(bf16)
    v_all[r, SEG:, :] = nn(m_sum[...], v_all[r, :SEG, :]).astype(bf16)


def project_kernel(info, x, gain, w_qkv, m_sum, m_mean, normed, q_all, k_all, v_all, ex):
    norm_phase(x, gain, normed)
    for r in range(x.shape[0]):
        project_phase(
            info, r, normed, lambda m: w_qkv[m * SEG : m * SEG + SEG, :], m_sum, m_mean, q_all, k_all, v_all
        )
        ex[0, r] = k_all[r, 2 * SEG - 32 :, :]
        ex[1, r] = v_all[r, 2 * SEG - 32 :, :]


def fill_bias(bias, bias7):
    q = iota((128, 256), 0)
    k = iota((128, 256), 1) & 127
    bias[0] = jnp.where((q >> 5) == (k >> 5), 0.0, NEG)
    bias[1] = jnp.where(((q >> 4) ^ (k >> 4)) == 1, 0.0, NEG)
    wide = bias7.shape[1] // 2
    q = iota((128, 2 * wide), 0)
    k = iota((128, 2 * wide), 1)
    k = jnp.where(k >= wide, k - wide, k)
    ok = (((q >> 4) ^ (k >> 4)) == 1) & (q < 96) & (k < 96)
    ok = ok | ((q >= 96) & (q < 112) & (k >= 96) & (k < 112))
    ok = ok | ((q >= 112) & (q < 120) & (k >= 112) & (k < 128))
    ok = ok | ((q >= 120) & (q < 124) & (k >= 128) & (k < 144))
    bias7[...] = jnp.where(ok, 0.0, NEG)


def fill_bias_t(bias, bias7):
    k = iota((256, 128), 0) & 127
    q = iota((256, 128), 1)
    bias[0] = jnp.where((q >> 5) == (k >> 5), 0.0, NEG)
    bias[1] = jnp.where(((q >> 4) ^ (k >> 4)) == 1, 0.0, NEG)
    wide = bias7.shape[0] // 2
    k = iota((2 * wide, 128), 0)
    k = jnp.where(k >= wide, k - wide, k)
    q = iota((2 * wide, 128), 1)
    ok = (((q >> 4) ^ (k >> 4)) == 1) & (q < 96) & (k < 96)
    ok = ok | ((q >= 96) & (q < 112) & (k >= 96) & (k < 112))
    ok = ok | ((q >= 112) & (q < 120) & (k >= 112) & (k < 128))
    ok = ok | ((q >= 120) & (q < 124) & (k >= 128) & (k < 144))
    bias7[...] = jnp.where(ok, 0.0, NEG)


def fill_counts(info, rows, remote, counts, counts_far):
    pos0 = info[rows]
    me = info[rows + 1]
    for r in range(rows):
        length = info[r]
        at = iota((SEG, 128), 0)
        counts[r, :SEG, :] = jnp.where(at + pos0 < length, 1.0, 0.0).astype(bf16)
        level, index = level_of(at)
        size = lax.shift_left(jnp.ones_like(level), level)
        start = pos0 + index * size
        counts[r, SEG:, :] = jnp.clip(length - start, 0, size).astype(f32).astype(bf16)
        for m in range(remote):
            size_m = 1 << (LOCAL + m)
            group = (me >> m) ^ 1
            start = group * ((1 << m) * SEG) + iota((16, 128), 0) * size_m
            counts_far[r, 16 * m : 16 * m + 16, :] = jnp.clip(length - start, 0, size_m).astype(f32).astype(bf16)


def pair_split(values, low):
    zero = jnp.zeros_like(values)
    return jnp.concatenate([jnp.where(low, values, zero), jnp.where(low, zero, values)], axis=0)


def last_rows(local, far, wide):
    parts = [local, far]
    rest = wide - local.shape[0] - far.shape[0]
    if rest:
        parts.append(jnp.zeros((rest, local.shape[1]), local.dtype))
    return jnp.concatenate(parts, axis=0)


def key_tile(t, r, lanes, k_all, v_all, counts, k_far, v_far, counts_far, wide):
    if t < 7:
        at = slice(128 * t, 128 * t + 128)
        return k_all[r, at, lanes], v_all[r, at, lanes], counts[r, at, :]
    at = slice(896, 992)
    return (
        last_rows(k_all[r, at, lanes], k_far[r, :, lanes], wide),
        last_rows(v_all[r, at, lanes], v_far[r, :, lanes], wide),
        last_rows(counts[r, at, :], counts_far[r], wide),
    )


def bias_of(t, bias, bias7):
    if t < 4:
        return bias[0]
    if t < 7:
        return bias[1]
    return bias7[...]


def attend_phase(
    q_all, k_all, v_all, k_far, v_far, u_sum, mixed, rden, counts, counts_far, bias, bias7, pyr, hook
):
    rows = q_all.shape[0]
    wide = bias7.shape[1] // 2
    low = iota((128, 128), 1) < HD
    low7 = iota((wide, 128), 1) < HD

    def step(it, _):
        hook(it)
        r = it // 4
        lanes = pl.ds(pl.multiple_of((it % 4) * 128, 128), 128)
        base = []
        for t in range(8):
            q = q_all[r, 128 * t : 128 * t + 128, lanes]
            k, v, c = key_tile(t, r, lanes, k_all, v_all, counts, k_far, v_far, counts_far, wide)
            lm = low if t < 7 else low7
            score = nt(q, pair_split(k, lm)) + bias_of(t, bias, bias7)
            weight = jnp.exp(score).astype(bf16)
            both = nn(weight, jnp.concatenate([pair_split(v, lm), pair_split(c, lm)], axis=1))
            if t < 4:
                base.append(both)
            else:
                pyr[128 * (t - 4) : 128 * (t - 4) + 128, :] = both.astype(bf16)
        for t in range(4):
            total = base[t] + nn(u_sum[128 * t : 128 * t + 128, :], pyr[...])
            inv = 1.0 / total[:, 128:]
            mixed[r, 128 * t : 128 * t + 128, lanes] = (total[:, :128] * inv).astype(bf16)
            rden[r, 128 * t : 128 * t + 128, lanes] = inv
        return 0

    lax.fori_loop(0, rows * 4, step, 0)


def no_hook(it):
    pass


def attend_kernel(
    info, q_all, k_all, v_all, k_far, v_far, u_sum, mixed, rden, counts, counts_far, bias, bias7, pyr
):
    fill_bias(bias, bias7)
    fill_counts(info, q_all.shape[0], k_far.shape[1] // 16, counts, counts_far)
    attend_phase(
        q_all, k_all, v_all, k_far, v_far, u_sum, mixed, rden, counts, counts_far, bias, bias7, pyr, no_hook
    )


CHUNK = 256


def token_chunks(rows):
    for r in range(rows):
        for c in range(SEG // CHUNK):
            yield r, c, slice(c * CHUNK, c * CHUNK + CHUNK), slice(r * SEG + c * CHUNK, r * SEG + c * CHUNK + CHUNK)


def fold(values):
    return values.reshape(values.shape[0] // 8, 8, values.shape[1]).sum(axis=0)


def residual_phase(info, x, mixed, cot, w_out, gain, res, hat, inv_s, n2, gout):
    rows = x.shape[0]
    for r, c, at, to in token_chunks(rows):
        value = x[r, at, :].astype(f32) + nn(mixed[r, at, :], w_out())
        res[to, :] = value
        h, s = norm_parts(value)
        hat[to, :] = h
        inv_s[to, :] = jnp.broadcast_to(s, (CHUNK, 128))
        n2[to, :] = (h * gain[...]).astype(bf16)
        pos = iota((CHUNK, SEG), 0) + (c * CHUNK + info[rows])
        gout[to, :] = jnp.where(pos < info[r], cot[r, at, :].astype(f32), 0.0).astype(bf16)


def ffn_phase(rows, count, n2, gout, w_hid, w_proj, b_hid, add_b, put_hid, put_proj, ffn, gn2, act_s, gpre_s, hook):
    def unit_step(f, _):
        hook(f)

        def token_step(c, _):
            to = pl.ds(pl.multiple_of(c * CHUNK, CHUNK), CHUNK)
            pre = nt(n2[to, :], w_hid(f)) + b_hid(f)
            k0 = 0.7978845608028654
            sq = pre * pre
            t = jnp.tanh(k0 * pre * (1.0 + 0.044715 * sq))
            half = 0.5 + 0.5 * t
            act = (pre * half).astype(bf16)
            slope = half + 0.5 * pre * (1.0 - t * t) * (k0 + (3.0 * 0.044715 * k0) * sq)
            gpre = (nt(gout[to, :], w_proj(f)) * slope).astype(bf16)
            act_s[to, :] = act
            gpre_s[to, :] = gpre
            add_b(f, fold(gpre.astype(f32)))
            add_f = nn(act, w_proj(f))
            add_g = nn(gpre, w_hid(f))

            @pl.when(f == 0)
            def _():
                ffn[to, :] = add_f
                gn2[to, :] = add_g

            @pl.when(f > 0)
            def _():
                ffn[to, :] = ffn[to, :] + add_f
                gn2[to, :] = gn2[to, :] + add_g

            return 0

        lax.fori_loop(0, rows * SEG // CHUNK, token_step, 0)
        put_proj(f, tn(act_s[...], gout[...]))
        put_hid(f, tn(gpre_s[...], n2[...]))
        return 0

    lax.fori_loop(0, count, unit_step, 0)


def output_phase(rows, res, hat, inv_s, gout, ffn, gn2, b_proj, gain, w_out, mixed, out, g_res, g_mixed, n2):
    sum_gain = jnp.zeros((8, SEG), f32)
    sum_out = jnp.zeros((8, SEG), f32)
    for r, c, at, to in token_chunks(rows):
        out[r, at, :] = (res[to, :] + ffn[to, :] + b_proj[...]).astype(bf16)
        go = gout[to, :].astype(f32)
        h = hat[to, :]
        g = gn2[to, :]
        sum_gain = sum_gain + fold(g * h)
        sum_out = sum_out + fold(go)
        inv = inv_s[to, :][:, :1]
        gr = go + norm_back(g, gain[...], h, inv)
        g_res[r, at, :] = gr
        grb = gr.astype(bf16)
        n2[to, :] = grb
        g_mixed[r, at, :] = nt(grb, w_out()).astype(bf16)
    acc = tn(mixed[0], n2[:SEG, :])
    for r in range(1, rows):
        acc = acc + tn(mixed[r], n2[r * SEG : r * SEG + SEG, :])
    return sum_gain, sum_out, acc


def ffn_kernel(
    info, x, mixed, cot, w_out, w_hid, w_proj, b_hid, b_proj, gain,
    out, g_res, g_mixed, gw_proj, gw_hid, gw_out, gb_hid, small,
    res, hat, inv_s, n2, gout, ffn, gn2, act_s, gpre_s,
):
    rows = x.shape[0]
    residual_phase(info, x, mixed, cot, lambda: w_out[...], gain, res, hat, inv_s, n2, gout)
    gb_hid[...] = jnp.zeros_like(gb_hid)

    def us(f):
        return pl.ds(pl.multiple_of(f * 512, 512), 512)

    def add_b(f, part):
        gb_hid[:, us(f)] = gb_hid[:, us(f)] + part

    def put_hid(f, value):
        gw_hid[us(f), :] = value

    def put_proj(f, value):
        gw_proj[us(f), :] = value

    ffn_phase(
        rows, w_hid.shape[0] // 512, n2, gout, lambda f: w_hid[us(f), :], lambda f: w_proj[us(f), :],
        lambda f: b_hid[:, us(f)], add_b, put_hid, put_proj, ffn, gn2, act_s, gpre_s, no_hook,
    )
    small[0], small[1], gw_out[...] = output_phase(
        rows, res, hat, inv_s, gout, ffn, gn2, b_proj, gain, lambda: w_out[...], mixed, out, g_res, g_mixed, n2
    )


def attend_back_phase(
    q_all, k_all, v_all, k_far, v_far, mixed, rden, g_mixed, m_sum, u_sum, u_mean, g_q, g_k, g_v, put_far,
    counts, counts_far, bias, bias7, bias_t, bias7_t, grad, gp_q, gp_k, gp_v, hook,
):
    rows = q_all.shape[0]
    remote = k_far.shape[1] // 16
    wide = bias7.shape[1] // 2
    low = iota((128, 128), 1) < HD
    low7 = iota((wide, 128), 1) < HD

    def step(it, _):
        hook(it)
        r = it // 4
        lanes = pl.ds(pl.multiple_of((it % 4) * 128, 128), 128)
        gnum = g_mixed[r, :, lanes].astype(f32) * rden[r, :, lanes]
        gden = -gnum * mixed[r, :, lanes].astype(f32)
        grad[:SEG, :] = jnp.concatenate([gnum, gden], axis=1).astype(bf16)
        grad[SEG:, :] = nn(m_sum[...], grad[:SEG, :]).astype(bf16)
        base_q, base_k, base_v = [], [], []
        for t in range(8):
            at = slice(128 * t, 128 * t + 128)
            q = q_all[r, at, lanes]
            k, v, c = key_tile(t, r, lanes, k_all, v_all, counts, k_far, v_far, counts_far, wide)
            lm = low if t < 7 else low7
            n_keys = 128 if t < 7 else wide
            g = grad[at, :]
            kk = pair_split(k, lm)
            vv = jnp.concatenate([pair_split(v, lm), pair_split(c, lm)], axis=1)
            weight = jnp.exp(nt(q, kk) + bias_of(t, bias, bias7))
            gs = (weight * nt(g, vv)).astype(bf16)
            gq = nn(gs, kk)
            weight_t = jnp.exp(nt(kk, q) + bias_of(t, bias_t, bias7_t))
            gs_t = (weight_t * nt(vv, g)).astype(bf16)
            gk = nn(gs_t, q)
            gv = nn(weight_t.astype(bf16), g[:, :128])
            gk = jnp.where(lm, gk[:n_keys], gk[n_keys:])
            gv = jnp.where(lm, gv[:n_keys], gv[n_keys:])
            if t < 4:
                base_q.append(gq)
                base_k.append(gk)
                base_v.append(gv)
            else:
                to = slice(128 * (t - 4), 128 * (t - 4) + 128)
                gp_q[to, :] = gq.astype(bf16)
                if t < 7:
                    gp_k[to, :] = gk.astype(bf16)
                    gp_v[to, :] = gv.astype(bf16)
                else:
                    gp_k[384:480, :] = gk[:96].astype(bf16)
                    gp_v[384:480, :] = gv[:96].astype(bf16)
                    gp_k[480:, :] = jnp.zeros((32, 128), bf16)
                    gp_v[480:, :] = jnp.zeros((32, 128), bf16)
                    put_far(r, lanes, gk[96 : 96 + 16 * remote], gv[96 : 96 + 16 * remote])
        for t in range(4):
            at = slice(128 * t, 128 * t + 128)
            to = pl.ds(pl.multiple_of(r * SEG + 128 * t, 128), 128)
            gq = (base_q[t] + nn(u_mean[at, :], gp_q[...])) * (HD**-0.5)
            g_q[to, lanes] = gq.astype(bf16)
            g_k[to, lanes] = base_k[t] + nn(u_mean[at, :], gp_k[...])
            g_v[to, lanes] = base_v[t] + nn(u_sum[at, :], gp_v[...])
        return 0

    lax.fori_loop(0, rows * 4, step, 0)


def attend_back_kernel(
    info, q_all, k_all, v_all, k_far, v_far, mixed, rden, g_mixed, m_sum, u_sum, u_mean,
    g_q, g_k, g_v, gk_far, gv_far,
    counts, counts_far, bias, bias7, bias_t, bias7_t, grad, gp_q, gp_k, gp_v,
):
    fill_bias(bias, bias7)
    fill_bias_t(bias_t, bias7_t)
    fill_counts(info, q_all.shape[0], k_far.shape[1] // 16, counts, counts_far)

    def put_far(r, lanes, gk, gv):
        gk_far[r, :, lanes] = gk.astype(bf16)
        gv_far[r, :, lanes] = gv.astype(bf16)

    attend_back_phase(
        q_all, k_all, v_all, k_far, v_far, mixed, rden, g_mixed, m_sum, u_sum, u_mean, g_q, g_k, g_v, put_far,
        counts, counts_far, bias, bias7, bias_t, bias7_t, grad, gp_q, gp_k, gp_v, no_hook,
    )


def key_grad_phase(info, rows, r, g_k, g_v, gk_in, gv_in, u_sum, u_mean, gkb, gvb):
    for c in range(SEG // CHUNK):
        at = slice(c * CHUNK, c * CHUNK + CHUNK)
        to = slice(r * SEG + c * CHUNK, r * SEG + c * CHUNK + CHUNK)
        gk = g_k[to, :] + nn(u_mean[at, 480:], gk_in)
        gv = g_v[to, :] + nn(u_sum[at, 480:], gv_in)
        pos = iota((CHUNK, SEG), 0) + (c * CHUNK + info[rows])
        gkb[to, :] = gk.astype(bf16)
        gvb[to, :] = jnp.where(pos < info[r], gv, 0.0).astype(bf16)


def qkv_grad(part, normed):
    rows = normed.shape[0]
    acc = tn(part[:SEG, :], normed[0])
    for r in range(1, rows):
        acc = acc + tn(part[r * SEG : r * SEG + SEG, :], normed[r])
    return acc


def input_grad_chunk(r, at, to, x, gain, weight, g_q, gkb, gvb, g_res, g_in):
    gn = nn(g_q[to, :], weight(0)) + nn(gkb[to, :], weight(1)) + nn(gvb[to, :], weight(2))
    h, inv = norm_parts(x[r, at, :].astype(f32))
    g_in[r, at, :] = g_res[r, at, :] + norm_back(gn, gain[...], h, inv)
    return fold(gn * h)


def finish_kernel(
    info, x, normed, gain, w_qkv, g_q, g_k, g_v, gk_in, gv_in, u_sum, u_mean, g_res,
    g_in, gw_qkv, small, gkb, gvb,
):
    rows = x.shape[0]
    for r in range(rows):
        key_grad_phase(info, rows, r, g_k, g_v, gk_in[r], gv_in[r], u_sum, u_mean, gkb, gvb)
    sum_gain = jnp.zeros((8, SEG), f32)
    for r, c, at, to in token_chunks(rows):
        sum_gain = sum_gain + input_grad_chunk(
            r, at, to, x, gain, lambda m: w_qkv[m * SEG : m * SEG + SEG, :], g_q, gkb, gvb, g_res, g_in
        )
    small[...] = sum_gain
    for part, src in enumerate((g_q, gkb, gvb)):
        gw_qkv[part * SEG : part * SEG + SEG, :] = qkv_grad(src, normed)


def sds(shape, dtype):
    return jax.ShapeDtypeStruct(shape, dtype)


def body_apart(
    inputs, lengths, attn_gain, w_query, w_key, w_value, w_output, ffn_gain, w_hidden, b_hidden,
    w_project, b_project, cotangent,
):
    seg, rows = inputs.shape[0], inputs.shape[1]
    assert seg == SEG and inputs.shape[2] == SEG
    heads = lax.axis_size("heads")
    dps = lax.axis_size("dp")
    remote = heads.bit_length() - 1
    me = lax.axis_index("heads")
    dp = lax.axis_index("dp")
    hw = w_query.shape[1]
    units = w_hidden.shape[1]
    info = jnp.concatenate([lengths, (me * SEG)[None], me[None]]).astype(jnp.int32)

    def gather(shard):
        piece = shard.reshape((dps, shard.shape[0] // dps, SEG))
        piece = lax.dynamic_index_in_dim(piece, dp, 0, keepdims=False)
        full = lax.all_gather(piece, "heads", axis=0)
        full = lax.all_gather(full, "dp", axis=1)
        return full.reshape((-1, SEG))

    local_qkv = jnp.stack([w_query.T, w_key.T, w_value.T])
    piece = local_qkv.reshape(3, dps, hw // dps, SEG)
    piece = lax.dynamic_index_in_dim(piece, dp, 1, keepdims=False)
    full = lax.all_gather(piece, "heads", axis=1)
    full = lax.all_gather(full, "dp", axis=2)
    w_qkv = full.reshape(3 * SEG, SEG)
    w_out = gather(w_output)
    w_hid = gather(w_hidden.T)
    w_proj = gather(w_project)
    b_hid = lax.all_gather(b_hidden.astype(f32), "heads", axis=0, tiled=True)[None, :]

    x = inputs.transpose(1, 0, 2)
    cot = cotangent.transpose(1, 0, 2)
    gain1 = attn_gain.astype(f32)[None, :]
    gain2 = ffn_gain.astype(f32)[None, :]
    b_proj = b_project.astype(f32)[None, :]
    m_sum, m_mean, u_sum, u_mean = pool_matrices()
    smem = pl.BlockSpec(memory_space=pltpu.SMEM)
    vec = pl.BlockSpec(memory_space=pltpu.VMEM)

    def call(kernel, outs, scratch, *args):
        return pl.pallas_call(
            kernel,
            out_shape=outs,
            in_specs=[smem] + [vec] * (len(args) - 1),
            out_specs=[vec] * len(outs),
            scratch_shapes=scratch,
            compiler_params=params(),
        )(*args)

    tok = (rows, SEG, SEG)
    pyr = (rows, 2 * SEG, SEG)
    normed, q_all, k_all, v_all, ex = call(
        project_kernel,
        [sds(tok, bf16), sds(pyr, bf16), sds(pyr, bf16), sds(pyr, bf16), sds((2, rows, 32, SEG), bf16)],
        [],
        info, x, gain1, w_qkv, m_sum, m_mean,
    )
    got = lax.all_gather(ex, "heads", axis=0)
    far = []
    for m in range(remote):
        group = (me >> m) ^ 1
        part = lax.dynamic_slice_in_dim(got, group << m, 1 << m, 0)
        first = 32 - (32 >> m)
        part = part[:, :, :, first : first + (16 >> m), :]
        far.append(part.transpose(1, 2, 0, 3, 4).reshape(2, rows, 16, SEG))
    far = jnp.concatenate(far, axis=2)
    k_far, v_far = far[0], far[1]

    wide = 128 * ((96 + 16 * remote + 127) // 128)
    att_scratch = [
        pltpu.VMEM((rows, 2 * SEG, 128), bf16),
        pltpu.VMEM((rows, 16 * remote, 128), bf16),
        pltpu.VMEM((2, 128, 256), f32),
        pltpu.VMEM((128, 2 * wide), f32),
    ]
    mixed, rden = call(
        attend_kernel,
        [sds(tok, bf16), sds(tok, f32)],
        att_scratch + [pltpu.VMEM((SEG, 256), bf16)],
        info, q_all, k_all, v_all, k_far, v_far, u_sum,
    )
    flat = (rows * SEG, SEG)
    ff = w_hid.shape[0]
    out, g_res, g_mixed, gw_proj, gw_hid, gw_out, gb_hid, small2 = call(
        ffn_kernel,
        [
            sds(tok, bf16), sds(tok, f32), sds(tok, bf16), sds((ff, SEG), f32), sds((ff, SEG), f32),
            sds((SEG, SEG), f32), sds((8, ff), f32), sds((2, 8, SEG), f32),
        ],
        [
            pltpu.VMEM(flat, f32), pltpu.VMEM(flat, f32), pltpu.VMEM((rows * SEG, 128), f32),
            pltpu.VMEM(flat, bf16), pltpu.VMEM(flat, bf16), pltpu.VMEM(flat, f32), pltpu.VMEM(flat, f32),
            pltpu.VMEM((rows * SEG, 512), bf16), pltpu.VMEM((rows * SEG, 512), bf16),
        ],
        info, x, mixed, cot, w_out, w_hid, w_proj, b_hid, b_proj, gain2,
    )

    def reduce(grad):
        mine = lax.psum_scatter(grad, ("heads", "dp"), scatter_dimension=0, tiled=True)
        return lax.all_gather(mine, "dp", axis=0, tiled=True)

    grad_ffn = reduce(jnp.stack([gw_hid, gw_proj], axis=0).reshape(2, heads, dps, units // dps, SEG)
                      .transpose(1, 2, 0, 3, 4).reshape(-1, SEG))
    grad_ffn = grad_ffn.reshape(dps, 2, units // dps, SEG).transpose(1, 0, 2, 3).reshape(2, units, SEG)

    g_q, g_k, g_v, gk_far, gv_far = call(
        attend_back_kernel,
        [
            sds(flat, bf16), sds(flat, f32), sds(flat, f32),
            sds((rows, 16 * remote, SEG), bf16), sds((rows, 16 * remote, SEG), bf16),
        ],
        att_scratch + [
            pltpu.VMEM((2, 256, 128), f32), pltpu.VMEM((2 * wide, 128), f32),
            pltpu.VMEM((2 * SEG, 256), bf16),
            pltpu.VMEM((SEG, 128), bf16), pltpu.VMEM((SEG, 128), bf16), pltpu.VMEM((SEG, 128), bf16),
        ],
        info, q_all, k_all, v_all, k_far, v_far, mixed, rden, g_mixed, m_sum, u_sum, u_mean,
    )
    back = lax.all_gather(jnp.stack([gk_far, gv_far]), "heads", axis=0)
    near = []
    for m in range(remote):
        group = (me >> m) ^ 1
        part = lax.dynamic_slice_in_dim(back, group << m, 1 << m, 0)
        part = part[:, :, :, 16 * m : 16 * m + 16, :].astype(f32).sum(axis=0)
        count = 16 >> m
        near.append(lax.dynamic_slice_in_dim(part, (me & ((1 << m) - 1)) * count, count, 2))
    pad = 32 - sum(p.shape[2] for p in near)
    near = jnp.concatenate(near + [jnp.zeros((2, rows, pad, SEG), f32)], axis=2).astype(bf16)

    g_in, gw_qkv, small1 = call(
        finish_kernel,
        [sds(tok, f32), sds((3 * SEG, SEG), f32), sds((8, SEG), f32)],
        [pltpu.VMEM(flat, bf16), pltpu.VMEM(flat, bf16)],
        info, x, normed, gain1, w_qkv, g_q, g_k, g_v, near[0], near[1], u_sum, u_mean, g_res,
    )
    every = jnp.concatenate([gw_qkv, gw_out], axis=0).reshape(4, heads, dps, hw // dps, SEG)
    grad_att = reduce(every.transpose(1, 2, 0, 3, 4).reshape(-1, SEG))
    grad_att = grad_att.reshape(dps, 4, hw // dps, SEG).transpose(1, 0, 2, 3).reshape(4, hw, SEG)

    tiny = jnp.concatenate([small1.sum(0), small2.sum(1).reshape(-1), gb_hid.sum(0)])
    tiny = lax.psum(tiny, ("dp", "heads"))
    gb = lax.dynamic_slice_in_dim(tiny[3 * SEG :], me * units, units, 0)
    return (
        out.transpose(1, 0, 2),
        g_in.transpose(1, 0, 2),
        tiny[:SEG],
        grad_att[0].T,
        grad_att[1].T,
        grad_att[2].T,
        grad_att[3],
        tiny[SEG : 2 * SEG],
        grad_ffn[0].T,
        gb,
        grad_ffn[1],
        tiny[2 * SEG : 3 * SEG],
    )


HEADS_FAST = 4
JOBS = (("qkv", 3, 16), ("out", 1, 16), ("hid", 1, 64), ("proj", 1, 64))
MESH = pl.DeviceIdType.MESH


class Info:
    def __init__(self, lengths, rows, me):
        self.lengths, self.rows, self.me = lengths, rows, me

    def __getitem__(self, at):
        if at < self.rows:
            return self.lengths[at]
        return self.me * SEG if at == self.rows else self.me


class Place:
    def __init__(self, send, recv):
        self.h = lax.axis_index("heads")
        self.dp = lax.axis_index("dp")
        self.c = lax.rem(self.dp, 2)
        self.x = lax.rem(self.dp // 2, 2)
        self.y = self.dp // 4
        self.send, self.recv = send, recv
        self.count = 0
        self.names = {}

    def partner(self):
        return {"dp": self.dp + 1 - 2 * self.c, "heads": self.h}

    def chip(self, k):
        x = self.x if k == 1 else 1 - self.x
        y = self.y if k == 0 else 1 - self.y
        return y, x, {"dp": y * 4 + x * 2 + self.c, "heads": self.h}

    def head(self, k):
        h = lax.rem(self.h + k, HEADS_FAST)
        return h, self.at_head(h)

    def at_head(self, h):
        return {"dp": self.dp, "heads": h}

    def slot(self, name):
        return self.names.setdefault(name, len(self.names))

    def copy(self, name, src, dst, device, arrives=None):
        at = self.slot(name)
        return pltpu.make_async_remote_copy(
            src_ref=src, dst_ref=dst, send_sem=self.send.at[at],
            recv_sem=self.recv.at[at if arrives is None else arrives],
            device_id=device, device_id_type=MESH,
        )


def start(copies):
    for copy in copies:
        copy.start()


def land(copies):
    for copy in copies:
        copy.wait_recv()


def sent(copies):
    for copy in copies:
        copy.wait_send()


class Gather:
    def __init__(self, p, name, own, full, local_sem):
        self.p, self.name, self.own, self.full, self.local_sem = p, name, own, full, local_sem

    def keep(self):
        p = self.p
        return pltpu.make_async_copy(
            self.own.at[:, p.y, p.x, p.c], self.full.at[:, p.h, p.y, p.x, p.c], self.local_sem
        )

    def along_heads(self):
        p = self.p
        for k in range(1, HEADS_FAST):
            yield p.copy(
                f"gz{self.name}{k}", self.own.at[:, p.y, p.x, p.c], self.full.at[:, p.h, p.y, p.x, p.c], p.head(k)[1]
            )

    def along_chips(self):
        p = self.p
        block = self.full.at[:, :, p.y, p.x, p.c]
        for k in range(3):
            yield p.copy(f"gx{self.name}{k}", block, block, p.chip(k)[2])

    def along_cores(self):
        p = self.p
        block = self.full.at[:, :, :, :, p.c]
        yield p.copy(f"gc{self.name}", block, block, p.partner())

    def step(self, at):
        if at == 0:
            self.keep().start()
            start(self.along_heads())
        elif at == 1:
            self.keep().wait()
            land(self.along_heads())
            start(self.along_chips())
        elif at == 2:
            land(self.along_chips())
            start(self.along_cores())
        else:
            land(self.along_cores())

    def close(self):
        sent(self.along_heads())
        sent(self.along_chips())
        sent(self.along_cores())


class Reduce:
    def __init__(self, p, name, grad, from_core, from_chip, from_head, total):
        self.p, self.name, self.grad, self.total = p, name, grad, total
        self.from_core, self.from_chip, self.from_head = from_core, from_chip, from_head

    def cores(self):
        p = self.p
        yield p.copy(f"rc{self.name}", self.grad.at[:, :, :, :, 1 - p.c], self.from_core, p.partner())

    def chips(self):
        p = self.p
        for k in range(3):
            y, x, device = p.chip(k)
            yield p.copy(f"rx{self.name}{k}", self.grad.at[:, :, y, x, p.c], self.from_chip.at[k], device)

    def heads(self):
        p = self.p
        for k in range(1, HEADS_FAST):
            h, device = p.head(k)
            yield p.copy(
                f"rz{self.name}{k}", self.grad.at[:, h, p.y, p.x, p.c], self.from_head.at[k - 1], device
            )

    def back_chips(self):
        p = self.p
        block = self.total.at[:, p.y, p.x, p.c]
        for k in range(3):
            yield p.copy(f"bx{self.name}{k}", block, block, p.chip(k)[2])

    def back_cores(self):
        p = self.p
        block = self.total.at[:, :, :, p.c]
        yield p.copy(f"bc{self.name}", block, block, p.partner())

    def step(self, at):
        p, grad = self.p, self.grad
        mats = grad.shape[0]
        if at == 0:
            start(self.cores())
        elif at == 1:
            land(self.cores())
            for m in range(mats):
                for h in range(HEADS_FAST):
                    both = grad[m, h, :, :, p.c].astype(f32) + self.from_core[m, h].astype(f32)
                    grad[m, h, :, :, p.c] = both.astype(bf16)
            start(self.chips())
        elif at == 2:
            land(self.chips())
            for m in range(mats):
                for h in range(HEADS_FAST):
                    acc = grad[m, h, p.y, p.x, p.c].astype(f32)
                    for k in range(3):
                        acc = acc + self.from_chip[k, m, h].astype(f32)
                    grad[m, h, p.y, p.x, p.c] = acc.astype(bf16)
            start(self.heads())
        elif at == 3:
            land(self.heads())
            for m in range(mats):
                acc = grad[m, p.h, p.y, p.x, p.c].astype(f32)
                for k in range(HEADS_FAST - 1):
                    acc = acc + self.from_head[k, m].astype(f32)
                self.total[m, p.y, p.x, p.c] = acc.astype(bf16)
            start(self.back_chips())
        elif at == 4:
            land(self.back_chips())
            start(self.back_cores())
        else:
            land(self.back_cores())

    def close(self):
        for part in (self.cores, self.chips, self.heads, self.back_chips, self.back_cores):
            sent(part())


class Small:
    def __init__(self, p, stage, from_core, from_chip, from_head):
        self.p, self.stage = p, stage
        self.from_core, self.from_chip, self.from_head = from_core, from_chip, from_head

    def cores(self):
        yield self.p.copy("sc", self.stage.at[0], self.from_core, self.p.partner())

    def chips(self):
        for k in range(3):
            yield self.p.copy(f"sx{k}", self.stage.at[1], self.from_chip.at[k], self.p.chip(k)[2])

    def heads(self):
        for k in range(1, HEADS_FAST):
            yield self.p.copy(f"sz{k}", self.stage.at[2], self.from_head.at[k - 1], self.p.head(k)[1])

    def step(self, at):
        if at == 0:
            start(self.cores())
        elif at == 1:
            land(self.cores())
            self.stage[1] = self.stage[0] + self.from_core[...]
            start(self.chips())
        elif at == 2:
            land(self.chips())
            self.stage[2] = self.stage[1] + self.from_chip[0] + self.from_chip[1] + self.from_chip[2]
            start(self.heads())
        else:
            land(self.heads())
            self.stage[3] = self.stage[2] + self.from_head[0] + self.from_head[1] + self.from_head[2]

    def close(self):
        for part in (self.cores, self.chips, self.heads):
            sent(part())


def whole_kernel(*refs, names):
    s = type("Refs", (), dict(zip(names, refs)))
    rows = s.x.shape[0]
    p = Place(s.send_sem, s.recv_sem)
    info = Info(s.lengths, rows, p.h)
    barrier = pltpu.get_barrier_semaphore()
    near = [p.partner()] + [p.chip(k)[2] for k in range(3)] + [p.head(k)[1] for k in range(1, HEADS_FAST)]
    for device in near:
        pl.semaphore_signal(barrier, inc=1, device_id=device, device_id_type=MESH)
    pl.semaphore_wait(barrier, len(near))

    gather = {
        name: Gather(p, name, getattr(s, "own_" + name), getattr(s, "w_" + name), s.local_sem.at[i])
        for i, (name, _, _) in enumerate(JOBS)
    }
    reduce = {
        name: Reduce(p, name, *(getattr(s, part + name) for part in ("g_", "rc_", "rx_", "rz_", "t_")))
        for name, _, _ in JOBS
    }
    small = Small(p, s.stage, s.small_c, s.small_x, s.small_z)

    def bias_copies():
        for k in range(1, HEADS_FAST):
            yield p.copy(f"bh{k}", s.b_own, s.b_all.at[p.h], p.head(k)[1])

    sib = p.h + 1 - 2 * lax.rem(p.h, 2)
    side = lax.rem(p.h, 2)
    other = 2 * (1 - p.h // 2)

    def far_copies(r, landing=False):
        for kv, src in enumerate((s.k_all, s.v_all)):
            yield p.copy(f"e5{r}{kv}", src.at[r, 992:1008], s.far.at[r, 0, kv], p.at_head(sib))
            base = [p.slot(f"e6{r}{kv}{d}") for d in range(2)][0]
            for d in range(2):
                to = d if landing else side
                dst = s.far.at[r, 1 + to, kv]
                yield p.copy(f"e6{r}{kv}{d}", src.at[r, 1008:1024], dst, p.at_head(other + d), base + to)

    def back_copies(r, landing=False):
        yield p.copy(f"f5{r}", s.g_far.at[r, 0], s.g_near.at[r, 0], p.at_head(sib))
        base = [p.slot(f"f6{r}{d}") for d in range(2)][0]
        for d in range(2):
            to = d if landing else side
            yield p.copy(f"f6{r}{d}", s.g_far.at[r, 1 + d], s.g_near.at[r, 1 + to], p.at_head(other + d), base + to)

    gather["qkv"].step(0)
    start(bias_copies())
    gather["out"].step(0)
    norm_phase(s.x, s.gain1, s.normed)
    s.b_all[p.h] = s.b_own[...]
    for i, kind in enumerate(((False, False), (False, True), (True, False), (True, True))):
        s.pools[i] = pool_matrix(*kind)
    m_sum, m_mean, u_sum, u_mean = (s.pools.at[i] for i in range(4))
    gather["hid"].step(0)
    gather["qkv"].step(1)
    gather["proj"].step(0)
    fill_bias(s.bias, s.bias7)
    fill_bias_t(s.bias_t, s.bias7_t)
    fill_counts(info, rows, 2, s.counts, s.counts_far)
    gather["out"].step(1)
    gather["qkv"].step(2)
    gather["hid"].step(1)
    gather["qkv"].step(3)

    def qkv_weight(m):
        return s.w_qkv[m].reshape(SEG, SEG)

    for r in range(rows):
        project_phase(info, r, s.normed, qkv_weight, m_sum, m_mean, s.q_all, s.k_all, s.v_all)
        start(far_copies(r))
        if r == 0:
            gather["proj"].step(1)
            gather["out"].step(2)

    def take_far(r):
        land(far_copies(r, True))
        for kv, dst in enumerate((s.k_far, s.v_far)):
            high = jnp.concatenate([s.far[r, 1, kv][:8], s.far[r, 2, kv][:8]], axis=0)
            dst[r] = jnp.concatenate([s.far[r, 0, kv], high], axis=0)

    def attend_hook(it):
        for r in range(rows):
            pl.when(it == 4 * r)(functools.partial(take_far, r))
        plan = {1: ("out", 3), 2: ("hid", 2), 4 * rows - 4: ("proj", 2), 4 * rows - 2: ("hid", 3)}
        for when, (name, step) in plan.items():
            pl.when(it == when)(functools.partial(gather[name].step, step))

    attend_phase(
        s.q_all, s.k_all, s.v_all, s.k_far, s.v_far, u_sum, s.mixed, s.rden, s.counts, s.counts_far,
        s.bias, s.bias7, s.pyr, attend_hook,
    )

    def out_weight():
        return s.w_out[0].reshape(SEG, SEG)

    residual_phase(info, s.x, s.mixed, s.cot, out_weight, s.gain2, s.res, s.hat, s.inv_s, s.n2, s.gout)
    gather["proj"].step(3)
    land(bias_copies())
    s.gb[...] = jnp.zeros_like(s.gb)

    def add_b(f, part):
        s.gb[f] = s.gb[f] + part

    def put(ref):
        def store(f, value):
            ref[0, f] = value.astype(bf16).reshape(ref.shape[2:])

        return store

    ffn_phase(
        rows, HEADS_FAST, s.n2, s.gout, lambda f: s.w_hid[0, f].reshape(512, SEG),
        lambda f: s.w_proj[0, f].reshape(512, SEG), lambda f: s.b_all[f][:1], add_b, put(s.g_hid), put(s.g_proj),
        s.ffn, s.gn2, s.act_s, s.gpre_s, no_hook,
    )
    reduce["proj"].step(0)
    reduce["hid"].step(0)
    sum_gain2, sum_out, acc = output_phase(
        rows, s.res, s.hat, s.inv_s, s.gout, s.ffn, s.gn2, s.b_proj, s.gain2, out_weight, s.mixed, s.out, s.g_in,
        s.g_mixed, s.n2,
    )
    s.g_out[0] = acc.astype(bf16).reshape(s.g_out.shape[1:])
    reduce["out"].step(0)

    def put_far(r, lanes, gk, gv):
        zero = jnp.zeros((8, 128), f32)
        for kv, g in enumerate((gk, gv)):
            s.g_far[r, 0, kv, :, lanes] = g[:16].astype(bf16)
            s.g_far[r, 1, kv, :, lanes] = jnp.concatenate([g[16:24], zero], axis=0).astype(bf16)
            s.g_far[r, 2, kv, :, lanes] = jnp.concatenate([g[24:32], zero], axis=0).astype(bf16)

    def back_hook(it):
        for r in range(1, rows):
            pl.when(it == 4 * r)(lambda r=r: start(back_copies(r - 1)))
        steps = 4 * rows
        plan = (
            (0, "proj", 1), (1, "hid", 1), (1, "out", 1), (steps // 2, "proj", 2), (steps - 3, "hid", 2),
            (steps - 2, "proj", 3), (steps - 2, "out", 2), (steps - 1, "hid", 3),
        )
        for when, name, step in plan:
            pl.when(it == when)(functools.partial(reduce[name].step, step))

    attend_back_phase(
        s.q_all, s.k_all, s.v_all, s.k_far, s.v_far, s.mixed, s.rden, s.g_mixed, m_sum, u_sum, u_mean,
        s.gpre_q, s.res, s.ffn, put_far, s.counts, s.counts_far, s.bias, s.bias7, s.bias_t, s.bias7_t, s.grad,
        s.gp_q, s.gp_k, s.gp_v, back_hook,
    )
    start(back_copies(rows - 1))
    s.g_qkv[0] = qkv_grad(s.gpre_q, s.normed).astype(bf16).reshape(s.g_qkv.shape[1:])
    reduce["out"].step(3)
    reduce["proj"].step(4)
    for r in range(rows):
        land(back_copies(r, True))
        near_in = []
        for kv in range(2):
            top = s.g_near[r, 1, kv][:8].astype(f32) + s.g_near[r, 2, kv][:8].astype(f32)
            top = jnp.concatenate([top, jnp.zeros((8, SEG), f32)], axis=0).astype(bf16)
            near_in.append(jnp.concatenate([s.g_near[r, 0, kv], top], axis=0))
        key_grad_phase(info, rows, r, s.res, s.ffn, *near_in, u_sum, u_mean, s.act_s, s.gpre_s)
    s.g_qkv[1] = qkv_grad(s.act_s, s.normed).astype(bf16).reshape(s.g_qkv.shape[1:])
    s.g_qkv[2] = qkv_grad(s.gpre_s, s.normed).astype(bf16).reshape(s.g_qkv.shape[1:])
    reduce["qkv"].step(0)
    reduce["hid"].step(4)
    sum_gain1 = jnp.zeros((8, SEG), f32)
    for i, (r, _, at, to) in enumerate(token_chunks(rows)):
        sum_gain1 = sum_gain1 + input_grad_chunk(
            r, at, to, s.x, s.gain1, qkv_weight, s.gpre_q, s.act_s, s.gpre_s, s.g_in, s.g_in
        )
        if i == 0:
            reduce["qkv"].step(1)
            reduce["out"].step(4)
    lines = [sum_gain1, sum_gain2, sum_out, jnp.zeros((8, SEG), f32)] + [s.gb[f] for f in range(HEADS_FAST)]
    s.stage[0] = jnp.concatenate([line.sum(axis=0, keepdims=True) for line in lines], axis=0)
    small.step(0)
    reduce["proj"].step(5)
    s.o_proj[...] = s.t_proj[0].reshape(512, SEG).astype(f32)
    small.step(1)
    reduce["hid"].step(5)
    s.o_hid[...] = s.t_hid[0].reshape(512, SEG).astype(f32).T
    reduce["qkv"].step(2)
    small.step(2)
    reduce["out"].step(5)
    s.o_out[...] = s.t_out[0].reshape(128, SEG).astype(f32)
    reduce["qkv"].step(3)
    small.step(3)
    s.o_gain1[...] = s.stage[3, 0:1, :]
    s.o_gain2[...] = s.stage[3, 1:2, :]
    s.o_bproj[...] = s.stage[3, 2:3, :]
    s.o_bhid[...] = s.stage[3, pl.ds(4 + p.h, 1), :]
    reduce["qkv"].step(4)
    reduce["qkv"].step(5)
    for m, ref in enumerate((s.o_q, s.o_k, s.o_v)):
        ref[...] = s.t_qkv[m].reshape(128, SEG).astype(f32).T
    for name, _, _ in JOBS:
        gather[name].close()
        reduce[name].close()
    small.close()
    sent(bias_copies())
    for r in range(rows):
        sent(far_copies(r))
        sent(back_copies(r))


def body_whole(
    inputs, lengths, attn_gain, w_query, w_key, w_value, w_output, ffn_gain, w_hidden, b_hidden,
    w_project, b_project, cotangent,
):
    rows = inputs.shape[1]
    tok, flat, pyr = (rows, SEG, SEG), (rows * SEG, SEG), (rows, 2 * SEG, SEG)
    operands = dict(
        lengths=lengths,
        x=inputs.transpose(1, 0, 2),
        cot=cotangent.transpose(1, 0, 2),
        gain1=attn_gain.astype(f32)[None, :],
        gain2=ffn_gain.astype(f32)[None, :],
        b_proj=b_project.astype(f32)[None, :],
        b_own=jnp.broadcast_to(b_hidden.astype(f32)[None, :], (8, 512)),
        own_qkv=jnp.stack([w_query.T, w_key.T, w_value.T]).reshape(3, 2, 2, 2, 16, SEG),
        own_out=w_output.reshape(1, 2, 2, 2, 16, SEG),
        own_hid=w_hidden.T.reshape(1, 2, 2, 2, 64, SEG),
        own_proj=w_project.reshape(1, 2, 2, 2, 64, SEG),
    )
    outs = dict(
        out=sds(tok, bf16), g_in=sds(tok, f32), o_gain1=sds((1, SEG), f32), o_q=sds((SEG, 128), f32),
        o_k=sds((SEG, 128), f32), o_v=sds((SEG, 128), f32), o_out=sds((128, SEG), f32), o_gain2=sds((1, SEG), f32),
        o_hid=sds((SEG, 512), f32), o_bhid=sds((1, 512), f32), o_proj=sds((512, SEG), f32), o_bproj=sds((1, SEG), f32),
    )
    v = pltpu.VMEM
    scratch = dict(
        b_all=v((HEADS_FAST, 8, 512), f32), normed=v(tok, bf16), pools=v((4, SEG, SEG), bf16),
        q_all=v(pyr, bf16), k_all=v(pyr, bf16), v_all=v(pyr, bf16), far=v((rows, 3, 2, 16, SEG), bf16),
        k_far=v((rows, 32, SEG), bf16), v_far=v((rows, 32, SEG), bf16), mixed=v(tok, bf16), rden=v(tok, f32),
        counts=v((rows, 2 * SEG, 128), bf16), counts_far=v((rows, 32, 128), bf16), bias=v((2, 128, 256), f32),
        bias7=v((128, 256), f32), bias_t=v((2, 256, 128), f32), bias7_t=v((256, 128), f32), pyr=v((SEG, 256), bf16),
        res=v(flat, f32), hat=v(flat, f32), inv_s=v((rows * SEG, 128), f32), n2=v(flat, bf16), gout=v(flat, bf16),
        ffn=v(flat, f32), gn2=v(flat, f32), act_s=v(flat, bf16), gpre_s=v(flat, bf16), gpre_q=v(flat, bf16),
        gb=v((HEADS_FAST, 8, 512), f32), g_mixed=v(tok, bf16), grad=v((2 * SEG, 256), bf16),
        gp_q=v((SEG, 128), bf16), gp_k=v((SEG, 128), bf16), gp_v=v((SEG, 128), bf16),
        g_far=v((rows, 3, 2, 16, SEG), bf16), g_near=v((rows, 3, 2, 16, SEG), bf16),
        stage=v((4, 8, SEG), f32), small_c=v((8, SEG), f32), small_x=v((3, 8, SEG), f32), small_z=v((3, 8, SEG), f32),
        local_sem=pltpu.SemaphoreType.DMA((4,)), send_sem=pltpu.SemaphoreType.DMA((128,)),
        recv_sem=pltpu.SemaphoreType.DMA((128,)),
    )
    for name, mats, piece in JOBS:
        scratch["w_" + name] = v((mats, HEADS_FAST, 2, 2, 2, piece, SEG), bf16)
        scratch["g_" + name] = v((mats, HEADS_FAST, 2, 2, 2, piece, SEG), bf16)
        scratch["rc_" + name] = v((mats, HEADS_FAST, 2, 2, piece, SEG), bf16)
        scratch["rx_" + name] = v((3, mats, HEADS_FAST, piece, SEG), bf16)
        scratch["rz_" + name] = v((3, mats, piece, SEG), bf16)
        scratch["t_" + name] = v((mats, 2, 2, 2, piece, SEG), bf16)
    names = tuple(operands) + tuple(outs) + tuple(scratch)
    vec = pl.BlockSpec(memory_space=pltpu.VMEM)
    got = pl.pallas_call(
        functools.partial(whole_kernel, names=names),
        out_shape=list(outs.values()),
        in_specs=[pl.BlockSpec(memory_space=pltpu.SMEM)] + [vec] * (len(operands) - 1),
        out_specs=[vec] * len(outs),
        scratch_shapes=list(scratch.values()),
        compiler_params=pltpu.CompilerParams(
            vmem_limit_bytes=67043328, collective_id=0, has_side_effects=True
        ),
    )(*operands.values())
    o = dict(zip(outs, got))
    return (
        o["out"].transpose(1, 0, 2), o["g_in"].transpose(1, 0, 2), o["o_gain1"][0], o["o_q"], o["o_k"], o["o_v"],
        o["o_out"], o["o_gain2"][0], o["o_hid"], o["o_bhid"][0], o["o_proj"], o["o_bproj"][0],
    )


def body(*args):
    fast = lax.axis_size("heads") == HEADS_FAST and lax.axis_size("dp") == 8
    fast = fast and args[3].shape[1] == 128 and args[8].shape[1] == 512
    return (body_whole if fast else body_apart)(*args)


def solution(mesh):
    rows = P("heads", "dp", None)
    cols, flat, tall = P(None, "heads"), P("heads"), P("heads", None)
    return jax.shard_map(
        body,
        mesh=mesh,
        in_specs=(rows, P("dp"), P(), cols, cols, cols, tall, P(), cols, flat, tall, P(), rows),
        out_specs=(rows, rows, P(), cols, cols, cols, tall, P(), cols, flat, tall, P()),
        check_vma=False,
    )
```
